32 devices in a mesh: dp: 32 (over z, y, x, core).
Axes of the slice: x: 2, y: 2, z: 4, core: 2. Of those that a mesh axis runs over, the one named last changes fastest.
Arguments:
- features: bfloat16 [32, 32, 8, 2048], P('dp'), may hold values from -12 to 14, as said below
- slot_mask: int32 [32, 32, 8], P('dp'), may hold values from 0 to 1, as said below
- owner: int32 [32], replicated, may hold values from 0 to 31, each once
Outputs:
- class_mean: float32 [32, 2048], P('dp')
- class_cov: float32 [32, 2048, 2048], P('dp')
The draws below stay inside these ranges and needn't reach their ends.
Inputs may be any that keep to these rules, and one draw needn't show every extreme that they name: `slot_mask`: every class has one device whose block of that class is full, so each class counts at least 8 images; about two thirds of slots hold images, with a fill rate that differs from class to class. The features of a class scatter around a class mean.
All inputs are finite; a program needn't handle non-finite values.
Results may differ from the reference program's by a relative error of at most 0.0003.
Values may be sent and summed in bfloat16 or wider, within the bound.
No kernel may reach another device: no remote copies, remote signals or barrier semaphores. Data moves between devices by JAX's collectives and lax.ppermute only.
A program may use at most 64 MiB of HBM per device.

```python
import math
import jax
import jax.numpy as jnp
from jax import lax

F = 2048
CAP = 8
CLASSES = 32
N_DP = 32


def draw_features(key, part):
    first, second, third = jax.random.split(jax.random.fold_in(key, 11), 3)
    offset = jax.random.uniform(first, (1, CLASSES, 1, F), jnp.float32, 0.0, 2.0)
    spread = jnp.exp(jax.random.uniform(second, (1, 1, 1, F), jnp.float32, math.log(0.3), math.log(3.0)))
    noise = jnp.clip(jax.random.normal(third, (N_DP, CLASSES, CAP, F), jnp.float32), -4.0, 4.0)
    return (offset + spread * noise).astype(jnp.bfloat16)


def draw_slot_mask(key, part):
    first, second, third = jax.random.split(jax.random.fold_in(key, 23), 3)
    level = jax.random.randint(first, (1, CLASSES, 1), 30, 96)
    rolls = jax.random.randint(second, (N_DP, CLASSES, CAP), 0, 100)
    filled = (rolls < level).astype(jnp.int32)
    full_at = jax.random.randint(third, (CLASSES,), 0, N_DP)
    hit = (jnp.arange(N_DP)[:, None] == full_at[None, :])[:, :, None]
    return jnp.where(hit, 1, filled).astype(jnp.int32)


def setup_inputs(seed: int = 0) -> dict:
    seeds = jax.random.split(jax.random.key(seed), 4)
    return {
        "features": draw_features(jax.random.fold_in(seeds[3], 71), 0),
        "slot_mask": draw_slot_mask(jax.random.fold_in(seeds[3], 71), 0),
        "owner": jax.random.permutation(seeds[2], CLASSES).astype(jnp.int32),
    }


def one_class(args):
    rows, weights = args
    rows = rows.reshape(-1, rows.shape[-1]).astype(jnp.float32)
    weights = weights.reshape(-1).astype(jnp.float32)
    count = jnp.sum(weights)
    mean = jnp.sum(rows * weights[:, None], axis=0) / count
    centered = (rows - mean[None, :]) * weights[:, None]
    cov = lax.dot_general(centered, centered, (((0,), (0,)), ((), ())), precision=lax.Precision.HIGHEST, preferred_element_type=jnp.float32)
    return mean, cov / (count - 1.0)


def reference(features, slot_mask, owner):
    devices = jnp.arange(CLASSES, dtype=jnp.int32)
    match = (owner[None, :] == devices[:, None]).astype(jnp.int32)
    class_of = jnp.sum(match * devices[None, :], axis=1).astype(jnp.int32)

    def per_owner(cls):
        rows = lax.dynamic_index_in_dim(features, cls, 1, keepdims=False)
        weights = lax.dynamic_index_in_dim(slot_mask, cls, 1, keepdims=False)
        return one_class((rows, weights))

    class_mean, class_cov = lax.map(per_owner, class_of)
    return class_mean, class_cov
```

```python
import functools

import jax
import jax.numpy as jnp
from jax import lax
from jax.experimental import pallas as pl
from jax.experimental.pallas import tpu as pltpu
from jax.sharding import PartitionSpec as P

LANES = 128
MARK = 2.0**100
LIMIT = 2.0**90


def pack_kernel(owner_ref, mask_ref, blocks_ref, out_ref):
    classes, slots, width = blocks_ref.shape
    mask = mask_ref[...].astype(jnp.float32)
    lane = lax.broadcasted_iota(jnp.int32, mask.shape, 1)

    def one(c, carry):
        weight = jnp.sum(jnp.where(lane == c, mask, 0.0), axis=1, keepdims=True)
        place = owner_ref[c]
        wide = jnp.broadcast_to(weight, (slots, LANES)).astype(jnp.bfloat16)
        mark = ((1.0 - weight) * MARK).astype(jnp.bfloat16)
        for j in range(0, width, LANES):
            tile = blocks_ref[c, :, j : j + LANES] * wide
            if j == 0:
                tile = tile + jnp.broadcast_to(mark, (slots, LANES))
            out_ref[place, :, j : j + LANES] = tile
        return carry

    lax.fori_loop(0, classes, one, 0, unroll=4)


def cov_kernel(rows_ref, mean_ref, cov_ref, clean, ones, shift, scal):
    step = pl.program_id(0)
    height = cov_ref.shape[1]

    @pl.when(step == 0)
    def _():
        first = rows_ref[:, :LANES]
        held = first.astype(jnp.float32) < LIMIT
        clean[:, :LANES] = jnp.where(held, first.astype(jnp.float32), 0.0).astype(jnp.bfloat16)
        clean[:, LANES:] = rows_ref[:, LANES:]
        weight = held.astype(jnp.float32)
        ones[...] = weight.astype(jnp.bfloat16)
        count = jnp.sum(weight, axis=0, keepdims=True)[:, :1]
        total = jnp.sum(clean[...].astype(jnp.float32), axis=0, keepdims=True)
        mean = total / count
        mean_ref[...] = mean
        shift[...] = mean / (count - 1.0)
        scal[...] = jnp.broadcast_to(1.0 / (count - 1.0), scal.shape)

    at = pl.ds(pl.multiple_of(step * height, height), height)
    left = clean[:, at]
    contract = (((0,), (0,)), ((), ()))
    second = lax.dot_general(left, clean[...], contract, preferred_element_type=jnp.float32)
    total = lax.dot_general(left, ones[...], contract, preferred_element_type=jnp.float32)[:, :1]
    cov_ref[0] = second * scal[:, :1] - total * shift[...]


def local(features, slot_mask, owner):
    blocks = features[0]
    classes, slots, width = blocks.shape
    mask = jnp.swapaxes(slot_mask[0], 0, 1)
    vmem = pl.BlockSpec(memory_space=pltpu.VMEM)
    packed = pl.pallas_call(
        pack_kernel,
        out_shape=jax.ShapeDtypeStruct(blocks.shape, blocks.dtype),
        in_specs=[pl.BlockSpec(memory_space=pltpu.SMEM), vmem, vmem],
        out_specs=vmem,
        name="pack",
    )(owner, mask, blocks)
    arrived = lax.all_to_all(packed, "dp", split_axis=0, concat_axis=0, tiled=True)
    rows = arrived.reshape(-1, width)
    depth = rows.shape[0]
    height = 128
    mean, cov = pl.pallas_call(
        cov_kernel,
        grid=(width // height,),
        out_shape=(
            jax.ShapeDtypeStruct((1, width), jnp.float32),
            jax.ShapeDtypeStruct((1, width, width), jnp.float32),
        ),
        in_specs=[pl.BlockSpec((depth, width), lambda i: (0, 0))],
        out_specs=(
            pl.BlockSpec((1, width), lambda i: (0, 0)),
            pl.BlockSpec((1, height, width), lambda i: (0, i, 0)),
        ),
        scratch_shapes=[
            pltpu.VMEM((depth, width), jnp.bfloat16),
            pltpu.VMEM((depth, LANES), jnp.bfloat16),
            pltpu.VMEM((1, width), jnp.float32),
            pltpu.VMEM((1, LANES), jnp.float32),
        ],
        name="covariance",
    )(rows)
    return mean, cov


def solution(mesh):
    return jax.shard_map(
        local,
        mesh=mesh,
        in_specs=(P("dp", None, None, None), P("dp", None, None), P()),
        out_specs=(P("dp", None), P("dp", None, None)),
        check_vma=False,
    )
```

```python
import jax
import jax.numpy as jnp
from jax import lax
from jax.experimental import pallas as pl
from jax.experimental.pallas import tpu as pltpu
from jax.sharding import PartitionSpec as P

LANES = 128
MARK = 2.0**100
LIMIT = 2.0**90
MIB = 2**20


def pack_kernel(groups, owner_hbm, mask_hbm, blocks_hbm, out_ref, owner, mask, blocks, wide, small, big):
    classes, slots, width = out_ref.shape
    each = classes // groups
    to_owner = pltpu.make_async_copy(owner_hbm, owner, small.at[0])
    to_mask = pltpu.make_async_copy(mask_hbm, mask, small.at[1])
    to_mask.start()
    to_owner.start()
    loads = []
    for g in range(groups):
        part = pl.ds(g * each, each)
        loads.append(pltpu.make_async_copy(blocks_hbm.at[part], blocks.at[part], big.at[g]))
        loads[-1].start()
    to_mask.wait()
    for c in range(classes):
        weight = mask[:, c : c + 1].astype(jnp.float32)
        wide[c] = jnp.broadcast_to(weight, (slots, LANES)).astype(jnp.bfloat16)
    to_owner.wait()
    for g in range(groups):
        loads[g].wait()

        def one(i, carry):
            c = g * each + i
            place = owner[c]
            weight = wide[c]
            for j in range(0, width, LANES):
                tile = blocks[c, :, j : j + LANES] * weight
                if j == 0:
                    tile = tile + (1.0 - weight) * MARK
                out_ref[place, :, j : j + LANES] = tile
            return carry

        lax.fori_loop(0, each, one, 0, unroll=min(4, each))


def cov_kernel(rows_ref, mean_ref, cov_ref, clean, ones, shift, scale, mean, left, out, mean_sem, cov_sem):
    depth, width = clean.shape
    first = rows_ref[:, :LANES].astype(jnp.float32)
    held = first < LIMIT
    clean[:, :LANES] = jnp.where(held, first, 0.0).astype(jnp.bfloat16)
    clean[:, LANES:] = rows_ref[:, LANES:]
    weight = held.astype(jnp.float32)
    ones[...] = weight.astype(jnp.bfloat16)
    count = jnp.sum(weight, axis=0, keepdims=True)
    scale[...] = 1.0 / (count - 1.0)
    for j in range(0, width, LANES):
        part = slice(j, j + LANES)
        total = jnp.sum(clean[:, part].astype(jnp.float32), axis=0, keepdims=True)
        mean[:, part] = total / count
        shift[:, part] = total / count * scale[...]
    mean_copy = pltpu.make_async_copy(mean, mean_ref, mean_sem)
    mean_copy.start()

    contract = (((1,), (0,)), ((), ()))
    tile = 2 * LANES

    def block(at, height):
        left[:height] = clean[:, pl.ds(at, height)].T
        total = lax.dot_general(left[:height], ones[...], contract, preferred_element_type=jnp.float32)
        for j in range(0, width, tile):
            second = lax.dot_general(
                left[:height], clean[:, j : j + tile], contract, preferred_element_type=jnp.float32
            )
            for k in range(0, tile, LANES):
                part = slice(j + k, j + k + LANES)
                out[pl.ds(at, height), part] = second[:, k : k + LANES] * scale[...] - total * shift[:, part]
        here = pl.ds(at, height)
        pltpu.make_async_copy(out.at[here], cov_ref.at[0, here], cov_sem).start()

    block(0, LANES)
    block(LANES, LANES)

    def step(i, carry):
        block(pl.multiple_of(i * tile, tile), tile)
        return carry

    lax.fori_loop(1, width // tile, step, 0)
    pltpu.make_async_copy(out, cov_ref.at[0], cov_sem).wait()
    mean_copy.wait()


def local(features, slot_mask, owner):
    blocks = features[0]
    classes, slots, width = blocks.shape
    mask = jnp.swapaxes(slot_mask[0], 0, 1)
    vmem = pl.BlockSpec(memory_space=pltpu.VMEM)
    hbm = pl.BlockSpec(memory_space=pltpu.HBM)
    groups = 4
    packed = pl.pallas_call(
        lambda *refs: pack_kernel(groups, *refs),
        out_shape=jax.ShapeDtypeStruct(blocks.shape, blocks.dtype),
        in_specs=[hbm, hbm, hbm],
        out_specs=vmem,
        scratch_shapes=[
            pltpu.SMEM((classes,), jnp.int32),
            pltpu.VMEM((slots, classes), jnp.int32),
            pltpu.VMEM(blocks.shape, blocks.dtype),
            pltpu.VMEM((classes, slots, LANES), blocks.dtype),
            pltpu.SemaphoreType.DMA((2,)),
            pltpu.SemaphoreType.DMA((groups,)),
        ],
        compiler_params=pltpu.CompilerParams(vmem_limit_bytes=16 * MIB),
        name="pack",
    )(*(pltpu.with_memory_space_constraint(a, pltpu.HBM) for a in (owner, mask, blocks)))
    arrived = lax.all_to_all(packed, "dp", split_axis=0, concat_axis=0, tiled=True)
    rows = arrived.reshape(-1, width)
    depth = rows.shape[0]
    mean, cov = pl.pallas_call(
        cov_kernel,
        out_shape=(
            jax.ShapeDtypeStruct((1, width), jnp.float32),
            jax.ShapeDtypeStruct((1, width, width), jnp.float32),
        ),
        in_specs=[vmem],
        out_specs=(hbm, hbm),
        scratch_shapes=[
            pltpu.VMEM((depth, width), jnp.bfloat16),
            pltpu.VMEM((depth, LANES), jnp.bfloat16),
            pltpu.VMEM((1, width), jnp.float32),
            pltpu.VMEM((1, LANES), jnp.float32),
            pltpu.VMEM((1, width), jnp.float32),
            pltpu.VMEM((2 * LANES, depth), jnp.bfloat16),
            pltpu.VMEM((width, width), jnp.float32),
            pltpu.SemaphoreType.DMA,
            pltpu.SemaphoreType.DMA,
        ],
        compiler_params=pltpu.CompilerParams(vmem_limit_bytes=40 * MIB),
        name="covariance",
    )(rows)
    return mean, cov


def solution(mesh):
    return jax.shard_map(
        local,
        mesh=mesh,
        in_specs=(P("dp", None, None, None), P("dp", None, None), P()),
        out_specs=(P("dp", None), P("dp", None, None)),
        check_vma=False,
    )
```

```python
import jax
import jax.numpy as jnp
from jax import lax
from jax.experimental import pallas as pl
from jax.experimental.pallas import tpu as pltpu
from jax.sharding import PartitionSpec as P


AXIS = "dp"
LANES = 128
TILE = 2 * LANES
MARK = 2.0**100
LIMIT = 2.0**90
MIB = 2**20

VMEM = pl.BlockSpec(memory_space=pltpu.VMEM)
HBM = pl.BlockSpec(memory_space=pltpu.HBM)


def factors(devices):
    bits = devices.bit_length() - 1
    assert devices == 1 << bits
    inner = 1 << (bits + 1) // 2
    return devices // inner, inner


def late_width(width):
    return width * 6 // 16 // LANES * LANES


def tiles(width):
    return [(at, min(TILE, width - at)) for at in range(0, width, TILE)]


def pack_kernel(groups, inner, lead, owner_hbm, mask_hbm, blocks_hbm, early_hbm, late_ref, lead_ref, owner, mask, blocks, wide, small, big, out_sem):
    classes, slots, width = blocks.shape
    early = early_hbm.shape[-1]
    each = classes // groups
    to_owner = pltpu.make_async_copy(owner_hbm, owner, small.at[0])
    to_mask = pltpu.make_async_copy(mask_hbm, mask, small.at[1])
    to_mask.start()
    to_owner.start()
    loads = []
    for g in range(groups):
        part = pl.ds(g * each, each)
        loads.append(pltpu.make_async_copy(blocks_hbm.at[part], blocks.at[part], big.at[g]))
        loads[-1].start()
    me = lax.axis_index(AXIS)
    to_mask.wait()
    for c in range(classes):
        weight = mask[:, c : c + 1].astype(jnp.float32)
        wide[c] = jnp.broadcast_to(weight, (slots, LANES)).astype(jnp.bfloat16)
    to_owner.wait()
    for g in range(groups):
        loads[g].wait()

        def one(i, carry):
            c = g * each + i
            weight = wide[c]
            for j in range(0, early, LANES):
                tile = blocks[c, :, j : j + LANES] * weight
                if j == 0:
                    tile = tile + (1.0 - weight) * MARK
                blocks[c, :, j : j + LANES] = tile
            return carry

        lax.fori_loop(0, each, one, 0, unroll=min(4, each))

        def send(i, carry):
            c = g * each + i
            pltpu.make_async_copy(blocks.at[c, :, pl.ds(0, early)], early_hbm.at[owner[c]], out_sem).start()
            return carry

        lax.fori_loop(0, each, send, 0, unroll=min(4, each))

    def sort(c, carry):
        flip = jnp.bitwise_xor(owner[c], me)
        d = flip // inner
        q = flip % inner
        weight = wide[c]
        for j in range(early, width, LANES):
            late_ref[q, d, :, j - early : j - early + LANES] = blocks[c, :, j : j + LANES] * weight

        @pl.when(d == lead)
        def _():
            lead_ref[q] = late_ref[q, d]

        return carry

    lax.fori_loop(0, classes, sort, 0, unroll=4)
    pltpu.make_async_copy(blocks.at[:, :, pl.ds(0, early)], early_hbm, out_sem).wait()


def mix_kernel(lead, late_ref, lead_ref, *outs):
    for q, out in enumerate(outs):
        for d in range(out.shape[0]):
            out[d] = lead_ref[q] if d == lead else late_ref[q, d]


def repack_kernel(inner, *refs):
    held, sends = refs[:inner], refs[inner:]
    for d, send in enumerate(sends):
        for q in range(inner):
            send[q] = held[q][d]


def dot(left, right):
    return lax.dot_general(left, right, (((1,), (0,)), ((), ())), preferred_element_type=jnp.float32)


def means_of(rows, each, mean, shift, scale, at=0):
    for j in range(0, rows.shape[1], LANES):
        part = slice(j, j + LANES)
        value = jnp.sum(rows[:, part].astype(jnp.float32), axis=0, keepdims=True) * each
        mean[:, at + j : at + j + LANES] = value
        shift[:, part] = value * scale


def early_kernel(rows_ref, mean_ref, cov_ref, clean, turned, ones, stats, shift, out, cov_sem):
    width = rows_ref.shape[1]
    first = rows_ref[:, :LANES].astype(jnp.float32)
    held = first < LIMIT
    weight = held.astype(jnp.float32)
    ones[...] = weight.astype(jnp.bfloat16)
    count = jnp.sum(weight, axis=0, keepdims=True)
    each = 1.0 / count
    scale = 1.0 / (count - 1.0)
    stats[0:1] = each
    stats[1:2] = scale
    clean[:, :LANES] = jnp.where(held, first, 0.0).astype(jnp.bfloat16)
    clean[:, LANES:] = rows_ref[:, LANES:]
    means_of(clean, each, mean_ref, shift, scale)

    def block(at, height):
        here = pl.ds(at, height)
        turned[here] = clean[:, here].T
        total = dot(turned[here], ones[...])
        for j, wide in tiles(width):
            second = dot(turned[here], clean[:, j : j + wide])
            for k in range(0, wide, LANES):
                part = slice(j + k, j + k + LANES)
                out[here, part] = second[:, k : k + LANES] * scale - total * shift[:, part]
        pltpu.make_async_copy(out.at[here], cov_ref.at[0, here, pl.ds(0, width)], cov_sem).start()

    def step(i, carry):
        block(pl.multiple_of(i * TILE, TILE), TILE)
        return carry

    lax.fori_loop(0, width // TILE, step, 0)
    if width % TILE:
        block(width // TILE * TILE, width % TILE)
    pltpu.make_async_copy(out, cov_ref.at[0, pl.ds(0, width), pl.ds(0, width)], cov_sem).wait()


def late_kernel(inner, pieces, *refs):
    clean, turned, ones, stats, early_mean = refs[:5]
    parts = refs[5 : 5 + pieces]
    _, mean_ref, cov_ref, gathered, tail, mean, shift, early_shift, left, right, low, mean_sem, cov_sem = refs[5 + pieces :]
    depth, early = clean.shape
    late = tail.shape[-1]
    me = lax.axis_index(AXIS)
    for d in range(pieces):
        for q in range(inner):
            gathered[jnp.bitwise_xor(me, d * inner + q)] = parts[d][q]
    tail[...] = gathered[...].reshape(depth, late)
    each = stats[0:1]
    scale = stats[1:2]
    means_of(tail, each, mean, shift, scale, early)

    def beside(at, height):
        here = pl.ds(at, height)
        total = dot(turned[here], ones[...])
        for j, wide in tiles(late):
            second = dot(turned[here], tail[:, j : j + wide])
            for k in range(0, wide, LANES):
                part = slice(j + k, j + k + LANES)
                right[here, part] = second[:, k : k + LANES] * scale - total * shift[:, part]
        pltpu.make_async_copy(right.at[here], cov_ref.at[0, here, pl.ds(early, late)], cov_sem).start()

    for at, height in tiles(early):
        beside(at, height)

    mean[:, :early] = early_mean[...]
    mean_copy = pltpu.make_async_copy(mean, mean_ref, mean_sem)
    mean_copy.start()
    for j in range(0, early, LANES):
        early_shift[:, j : j + LANES] = early_mean[:, j : j + LANES] * scale

    def below(at, height):
        here = pl.ds(at, height)
        left[:height] = tail[:, here].T
        total = dot(left[:height], ones[...])
        for source, sums, base, span in ((clean, early_shift, 0, early), (tail, shift, early, late)):
            for j, wide in tiles(span):
                second = dot(left[:height], source[:, j : j + wide])
                for k in range(0, wide, LANES):
                    part = slice(j + k, j + k + LANES)
                    value = second[:, k : k + LANES] * scale - total * sums[:, part]
                    low[here, base + j + k : base + j + k + LANES] = value
        pltpu.make_async_copy(low.at[here], cov_ref.at[0, pl.ds(early + at, height)], cov_sem).start()

    for at, height in tiles(late):
        below(at, height)
    pltpu.make_async_copy(right, cov_ref.at[0, pl.ds(0, early), pl.ds(early, late)], cov_sem).wait()
    pltpu.make_async_copy(low, cov_ref.at[0, pl.ds(early, late)], cov_sem).wait()
    mean_copy.wait()


def local(features, slot_mask, owner):
    devices = lax.axis_size(AXIS)
    outer, inner = factors(devices)
    blocks = features[0]
    classes, slots, width = blocks.shape
    late = late_width(width)
    early = width - late
    depth = devices * slots
    bf16, f32 = jnp.bfloat16, jnp.float32
    mask = jnp.swapaxes(slot_mask[0], 0, 1)
    groups = 8

    inputs = [pltpu.with_memory_space_constraint(a, pltpu.HBM) for a in (owner, mask, blocks)]

    lead = outer // 2
    packed, sorted_late, leading = pl.pallas_call(
        lambda *refs: pack_kernel(groups, inner, lead, *refs),
        out_shape=(
            jax.ShapeDtypeStruct((devices, slots, early), bf16),
            jax.ShapeDtypeStruct((inner, outer, slots, late), bf16),
            jax.ShapeDtypeStruct((inner, slots, late), bf16),
        ),
        in_specs=[HBM, HBM, HBM],
        out_specs=(HBM, VMEM, VMEM),
        scratch_shapes=[
            pltpu.SMEM((classes,), jnp.int32),
            pltpu.VMEM((slots, classes), jnp.int32),
            pltpu.VMEM(blocks.shape, bf16),
            pltpu.VMEM((classes, slots, LANES), bf16),
            pltpu.SemaphoreType.DMA((2,)),
            pltpu.SemaphoreType.DMA((groups,)),
            pltpu.SemaphoreType.DMA,
        ],
        compiler_params=pltpu.CompilerParams(vmem_limit_bytes=16 * MIB),
        name="pack",
    )(*inputs)

    def far(d, value):
        return lax.ppermute(value, AXIS, [(i, i ^ (d * inner)) for i in range(devices)])

    led = far(lead, leading)
    arrived = lax.all_to_all(packed, AXIS, split_axis=0, concat_axis=0, tiled=True)
    mixed = pl.pallas_call(
        lambda *refs: mix_kernel(lead, *refs),
        out_shape=(jax.ShapeDtypeStruct((outer, slots, late), bf16),) * inner,
        in_specs=[VMEM] * 2,
        out_specs=(VMEM,) * inner,
        compiler_params=pltpu.CompilerParams(vmem_limit_bytes=16 * MIB),
        name="mix",
    )(sorted_late, led)
    held = [mixed[0]]
    for q in range(1, inner):
        held.append(lax.ppermute(mixed[q], AXIS, [(i, i ^ q) for i in range(devices)]))
    parts = pl.pallas_call(
        lambda *refs: repack_kernel(inner, *refs),
        out_shape=(jax.ShapeDtypeStruct((inner, slots, late), bf16),) * outer,
        in_specs=[VMEM] * inner,
        out_specs=(VMEM,) * outer,
        compiler_params=pltpu.CompilerParams(vmem_limit_bytes=16 * MIB),
        name="repack",
    )(*held)
    parts = [part if d in (0, lead) else far(d, part) for d, part in enumerate(parts)]
    rows = arrived.reshape(depth, early)
    early_mean, begun, *prepared = pl.pallas_call(
        early_kernel,
        out_shape=(
            jax.ShapeDtypeStruct((1, early), f32),
            jax.ShapeDtypeStruct((1, width, width), f32),
            jax.ShapeDtypeStruct((depth, early), bf16),
            jax.ShapeDtypeStruct((early, depth), bf16),
            jax.ShapeDtypeStruct((depth, LANES), bf16),
            jax.ShapeDtypeStruct((8, LANES), f32),
        ),
        in_specs=[VMEM],
        out_specs=(VMEM, HBM, VMEM, VMEM, VMEM, VMEM),
        scratch_shapes=[
            pltpu.VMEM((1, early), f32),
            pltpu.VMEM((early, early), f32),
            pltpu.SemaphoreType.DMA,
        ],
        compiler_params=pltpu.CompilerParams(vmem_limit_bytes=40 * MIB),
        cost_estimate=pl.CostEstimate(
            flops=2 * depth * early * early, bytes_accessed=4 * early * early, transcendentals=0
        ),
        name="early_covariance",
    )(rows)
    mean, cov = pl.pallas_call(
        lambda *refs: late_kernel(inner, outer, *refs),
        out_shape=(
            jax.ShapeDtypeStruct((1, width), f32),
            jax.ShapeDtypeStruct((1, width, width), f32),
        ),
        in_specs=[VMEM] * (5 + outer) + [HBM],
        out_specs=(HBM, HBM),
        scratch_shapes=[
            pltpu.VMEM((devices, slots, late), bf16),
            pltpu.VMEM((depth, late), bf16),
            pltpu.VMEM((1, width), f32),
            pltpu.VMEM((1, late), f32),
            pltpu.VMEM((1, early), f32),
            pltpu.VMEM((TILE, depth), bf16),
            pltpu.VMEM((early, late), f32),
            pltpu.VMEM((late, width), f32),
            pltpu.SemaphoreType.DMA,
            pltpu.SemaphoreType.DMA,
        ],
        input_output_aliases={5 + outer: 1},
        compiler_params=pltpu.CompilerParams(vmem_limit_bytes=40 * MIB),
        cost_estimate=pl.CostEstimate(
            flops=2 * depth * (width * width - early * early),
            bytes_accessed=4 * (width * width - early * early),
            transcendentals=0,
        ),
        name="late_covariance",
    )(*prepared, early_mean, *parts, begun)
    return mean, cov


def solution(mesh):
    return jax.shard_map(
        local,
        mesh=mesh,
        in_specs=(P(AXIS, None, None, None), P(AXIS, None, None), P()),
        out_specs=(P(AXIS, None), P(AXIS, None, None)),
        check_vma=False,
    )
```

```python
import jax
import jax.numpy as jnp
from jax import lax
from jax.experimental import pallas as pl
from jax.experimental.pallas import tpu as pltpu
from jax.sharding import PartitionSpec as P


AXIS = "dp"
LANES = 128
TILE = 2 * LANES
MARK = 2.0**100
LIMIT = 2.0**90
MIB = 2**20

VMEM = pl.BlockSpec(memory_space=pltpu.VMEM)
HBM = pl.BlockSpec(memory_space=pltpu.HBM)


def factors(devices):
    bits = devices.bit_length() - 1
    assert devices == 1 << bits
    inner = 1 << (bits + 1) // 2
    return devices // inner, inner


def leading_flips(outer):
    return [1 << bit for bit in reversed(range(outer.bit_length() - 1))]


def late_width(width):
    return width * 7 // 16 // LANES * LANES


def tiles(width):
    return [(at, min(TILE, width - at)) for at in range(0, width, TILE)]


def pack_kernel(groups, inner, leads, owner_hbm, mask_hbm, blocks_hbm, early_hbm, late_ref, *refs):
    lead_refs = refs[: len(leads)]
    owner, mask, blocks, wide, small, big, out_sem = refs[len(leads) :]
    classes, slots, width = blocks.shape
    early = early_hbm.shape[-1]
    each = classes // groups
    to_owner = pltpu.make_async_copy(owner_hbm, owner, small.at[0])
    to_mask = pltpu.make_async_copy(mask_hbm, mask, small.at[1])
    to_mask.start()
    to_owner.start()
    loads = []
    for g in range(groups):
        part = pl.ds(g * each, each)
        loads.append(pltpu.make_async_copy(blocks_hbm.at[part], blocks.at[part], big.at[g]))
        loads[-1].start()
    me = lax.axis_index(AXIS)
    to_mask.wait()
    for c in range(classes):
        weight = mask[:, c : c + 1].astype(jnp.float32)
        wide[c] = jnp.broadcast_to(weight, (slots, LANES)).astype(jnp.bfloat16)
    to_owner.wait()
    for g in range(groups):
        loads[g].wait()

        def one(i, carry):
            c = g * each + i
            weight = wide[c]
            for j in range(0, early, LANES):
                tile = blocks[c, :, j : j + LANES] * weight
                if j == 0:
                    tile = tile + (1.0 - weight) * MARK
                blocks[c, :, j : j + LANES] = tile
            return carry

        lax.fori_loop(0, each, one, 0, unroll=min(4, each))

        def send(i, carry):
            c = g * each + i
            pltpu.make_async_copy(blocks.at[c, :, pl.ds(0, early)], early_hbm.at[owner[c]], out_sem).start()
            return carry

        lax.fori_loop(0, each, send, 0, unroll=min(4, each))

    def sort(c, carry):
        flip = jnp.bitwise_xor(owner[c], me)
        d = flip // inner
        q = flip % inner
        weight = wide[c]
        for j in range(early, width, LANES):
            late_ref[q, d, :, j - early : j - early + LANES] = blocks[c, :, j : j + LANES] * weight

        for lead, lead_ref in zip(leads, lead_refs):

            @pl.when(d == lead)
            def _(lead_ref=lead_ref):
                lead_ref[q] = late_ref[q, d]

        return carry

    lax.fori_loop(0, classes, sort, 0, unroll=4)
    pltpu.make_async_copy(blocks.at[:, :, pl.ds(0, early)], early_hbm, out_sem).wait()


def mix_kernel(leads, late_ref, *refs):
    came = dict(zip(leads, refs))
    for q, out in enumerate(refs[len(leads) :]):
        for d in range(out.shape[0]):
            out[d] = came[d][q] if d in came else late_ref[q, d]


def repack_kernel(inner, *refs):
    held, sends = refs[:inner], refs[inner:]
    for d, send in enumerate(sends):
        for q in range(inner):
            send[q] = held[q][d]


def dot(left, right):
    return lax.dot_general(left, right, (((1,), (0,)), ((), ())), preferred_element_type=jnp.float32)


def means_of(rows, each, mean, shift, scale, at=0):
    for j in range(0, rows.shape[1], LANES):
        part = slice(j, j + LANES)
        value = jnp.sum(rows[:, part].astype(jnp.float32), axis=0, keepdims=True) * each
        mean[:, at + j : at + j + LANES] = value
        shift[:, part] = value * scale


def early_kernel(rows_ref, mean_ref, cov_ref, clean, turned, ones, stats, shift, out, cov_sem):
    width = rows_ref.shape[1]
    first = rows_ref[:, :LANES].astype(jnp.float32)
    held = first < LIMIT
    weight = held.astype(jnp.float32)
    ones[...] = weight.astype(jnp.bfloat16)
    count = jnp.sum(weight, axis=0, keepdims=True)
    each = 1.0 / count
    scale = 1.0 / (count - 1.0)
    stats[0:1] = each
    stats[1:2] = scale
    clean[:, :LANES] = jnp.where(held, first, 0.0).astype(jnp.bfloat16)
    clean[:, LANES:] = rows_ref[:, LANES:]
    means_of(clean, each, mean_ref, shift, scale)

    def block(at, height):
        here = pl.ds(at, height)
        turned[here] = clean[:, here].T
        total = dot(turned[here], ones[...])
        for j, wide in tiles(width):
            second = dot(turned[here], clean[:, j : j + wide])
            for k in range(0, wide, LANES):
                part = slice(j + k, j + k + LANES)
                out[here, part] = second[:, k : k + LANES] * scale - total * shift[:, part]
        pltpu.make_async_copy(out.at[here], cov_ref.at[0, here, pl.ds(0, width)], cov_sem).start()

    for at, height in tiles(width):
        block(at, height)
    pltpu.make_async_copy(out, cov_ref.at[0, pl.ds(0, width), pl.ds(0, width)], cov_sem).wait()


def late_kernel(inner, pieces, *refs):
    clean, turned, ones, stats, early_mean = refs[:5]
    parts = refs[5 : 5 + pieces]
    _, mean_ref, cov_ref, gathered, tail, mean, shift, early_shift, left, right, low, mean_sem, cov_sem = refs[5 + pieces :]
    depth, early = clean.shape
    late = tail.shape[-1]
    me = lax.axis_index(AXIS)
    for d in range(pieces):
        for q in range(inner):
            gathered[jnp.bitwise_xor(me, d * inner + q)] = parts[d][q]
    tail[...] = gathered[...].reshape(depth, late)
    each = stats[0:1]
    scale = stats[1:2]
    means_of(tail, each, mean, shift, scale, early)

    def beside(at, height):
        here = pl.ds(at, height)
        total = dot(turned[here], ones[...])
        for j, wide in tiles(late):
            second = dot(turned[here], tail[:, j : j + wide])
            for k in range(0, wide, LANES):
                part = slice(j + k, j + k + LANES)
                right[here, part] = second[:, k : k + LANES] * scale - total * shift[:, part]
        pltpu.make_async_copy(right.at[here], cov_ref.at[0, here, pl.ds(early, late)], cov_sem).start()

    for at, height in tiles(early):
        beside(at, height)

    mean[:, :early] = early_mean[...]
    mean_copy = pltpu.make_async_copy(mean, mean_ref, mean_sem)
    mean_copy.start()
    for j in range(0, early, LANES):
        early_shift[:, j : j + LANES] = early_mean[:, j : j + LANES] * scale

    def below(at, height):
        here = pl.ds(at, height)
        left[:height] = tail[:, here].T
        total = dot(left[:height], ones[...])
        for source, sums, base, span in ((clean, early_shift, 0, early), (tail, shift, early, late)):
            for j, wide in tiles(span):
                second = dot(left[:height], source[:, j : j + wide])
                for k in range(0, wide, LANES):
                    part = slice(j + k, j + k + LANES)
                    value = second[:, k : k + LANES] * scale - total * sums[:, part]
                    low[here, base + j + k : base + j + k + LANES] = value
        pltpu.make_async_copy(low.at[here], cov_ref.at[0, pl.ds(early + at, height)], cov_sem).start()

    for at, height in tiles(late):
        below(at, height)
    pltpu.make_async_copy(right, cov_ref.at[0, pl.ds(0, early), pl.ds(early, late)], cov_sem).wait()
    pltpu.make_async_copy(low, cov_ref.at[0, pl.ds(early, late)], cov_sem).wait()
    mean_copy.wait()


def local(features, slot_mask, owner):
    devices = lax.axis_size(AXIS)
    outer, inner = factors(devices)
    blocks = features[0]
    classes, slots, width = blocks.shape
    late = late_width(width)
    early = width - late
    depth = devices * slots
    bf16, f32 = jnp.bfloat16, jnp.float32
    mask = jnp.swapaxes(slot_mask[0], 0, 1)
    groups = 4

    inputs = [pltpu.with_memory_space_constraint(a, pltpu.HBM) for a in (owner, mask, blocks)]

    leads = leading_flips(outer)
    packed, sorted_late, *leading = pl.pallas_call(
        lambda *refs: pack_kernel(groups, inner, leads, *refs),
        out_shape=(
            jax.ShapeDtypeStruct((devices, slots, early), bf16),
            jax.ShapeDtypeStruct((inner, outer, slots, late), bf16),
        )
        + (jax.ShapeDtypeStruct((inner, slots, late), bf16),) * len(leads),
        in_specs=[HBM, HBM, HBM],
        out_specs=(HBM,) + (VMEM,) * (1 + len(leads)),
        scratch_shapes=[
            pltpu.SMEM((classes,), jnp.int32),
            pltpu.VMEM((slots, classes), jnp.int32),
            pltpu.VMEM(blocks.shape, bf16),
            pltpu.VMEM((classes, slots, LANES), bf16),
            pltpu.SemaphoreType.DMA((2,)),
            pltpu.SemaphoreType.DMA((groups,)),
            pltpu.SemaphoreType.DMA,
        ],
        compiler_params=pltpu.CompilerParams(vmem_limit_bytes=16 * MIB),
        name="pack",
    )(*inputs)

    def far(d, value):
        return lax.ppermute(value, AXIS, [(i, i ^ (d * inner)) for i in range(devices)])

    led = [far(d, value) for d, value in zip(leads, leading)]
    arrived = lax.all_to_all(packed, AXIS, split_axis=0, concat_axis=0, tiled=True)
    mixed = pl.pallas_call(
        lambda *refs: mix_kernel(leads, *refs),
        out_shape=(jax.ShapeDtypeStruct((outer, slots, late), bf16),) * inner,
        in_specs=[VMEM] * (1 + len(leads)),
        out_specs=(VMEM,) * inner,
        compiler_params=pltpu.CompilerParams(vmem_limit_bytes=16 * MIB),
        name="mix",
    )(sorted_late, *led)
    held = [mixed[0]]
    for q in range(1, inner):
        held.append(lax.ppermute(mixed[q], AXIS, [(i, i ^ q) for i in range(devices)]))
    parts = pl.pallas_call(
        lambda *refs: repack_kernel(inner, *refs),
        out_shape=(jax.ShapeDtypeStruct((inner, slots, late), bf16),) * outer,
        in_specs=[VMEM] * inner,
        out_specs=(VMEM,) * outer,
        compiler_params=pltpu.CompilerParams(vmem_limit_bytes=16 * MIB),
        name="repack",
    )(*held)
    parts = [part if d in (0, *leads) else far(d, part) for d, part in enumerate(parts)]
    rows = arrived.reshape(depth, early)
    early_mean, begun, *prepared = pl.pallas_call(
        early_kernel,
        out_shape=(
            jax.ShapeDtypeStruct((1, early), f32),
            jax.ShapeDtypeStruct((1, width, width), f32),
            jax.ShapeDtypeStruct((depth, early), bf16),
            jax.ShapeDtypeStruct((early, depth), bf16),
            jax.ShapeDtypeStruct((depth, LANES), bf16),
            jax.ShapeDtypeStruct((8, LANES), f32),
        ),
        in_specs=[VMEM],
        out_specs=(VMEM, HBM, VMEM, VMEM, VMEM, VMEM),
        scratch_shapes=[
            pltpu.VMEM((1, early), f32),
            pltpu.VMEM((early, early), f32),
            pltpu.SemaphoreType.DMA,
        ],
        compiler_params=pltpu.CompilerParams(vmem_limit_bytes=40 * MIB),
        cost_estimate=pl.CostEstimate(
            flops=2 * depth * early * early, bytes_accessed=4 * early * early, transcendentals=0
        ),
        name="early_covariance",
    )(rows)
    mean, cov = pl.pallas_call(
        lambda *refs: late_kernel(inner, outer, *refs),
        out_shape=(
            jax.ShapeDtypeStruct((1, width), f32),
            jax.ShapeDtypeStruct((1, width, width), f32),
        ),
        in_specs=[VMEM] * (5 + outer) + [HBM],
        out_specs=(HBM, HBM),
        scratch_shapes=[
            pltpu.VMEM((devices, slots, late), bf16),
            pltpu.VMEM((depth, late), bf16),
            pltpu.VMEM((1, width), f32),
            pltpu.VMEM((1, late), f32),
            pltpu.VMEM((1, early), f32),
            pltpu.VMEM((TILE, depth), bf16),
            pltpu.VMEM((early, late), f32),
            pltpu.VMEM((late, width), f32),
            pltpu.SemaphoreType.DMA,
            pltpu.SemaphoreType.DMA,
        ],
        input_output_aliases={5 + outer: 1},
        compiler_params=pltpu.CompilerParams(vmem_limit_bytes=40 * MIB),
        cost_estimate=pl.CostEstimate(
            flops=2 * depth * (width * width - early * early),
            bytes_accessed=4 * (width * width - early * early),
            transcendentals=0,
        ),
        name="late_covariance",
    )(*prepared, early_mean, *parts, begun)
    return mean, cov


def solution(mesh):
    return jax.shard_map(
        local,
        mesh=mesh,
        in_specs=(P(AXIS, None, None, None), P(AXIS, None, None), P()),
        out_specs=(P(AXIS, None), P(AXIS, None, None)),
        check_vma=False,
    )
```
